256 devices in a mesh: row: 8 (over x, core), col: 32 (over z, y).
Axes of the slice: x: 4, y: 4, z: 8, core: 2. Of those that a mesh axis runs over, the one named last changes fastest.
Arguments:
- trailing: float32 [16384, 16384], P('row', 'col'), may hold values from -9 to 9
- panel: float32 [16384, 256], P('row'), may hold values from -21 to 21
Outputs:
- updated: float32 [16384, 16384], P('row', 'col')
- band: float32 [256, 256], replicated
The draws below stay inside these ranges and needn't reach their ends.
All inputs are finite; a program needn't handle non-finite values.
Results may differ from the reference program's by a relative error of at most 0.0003.
Values sent between devices are 32-bit elements; how exact they have to be, the bound alone decides.
No kernel may reach another device: no remote copies, remote signals or barrier semaphores. Data moves between devices by JAX's collectives and lax.ppermute only.
A program may use at most 128 MiB of HBM per device.

```python
import jax
import jax.numpy as jnp
from jax import lax

M = 16384
B = 256


def draw_trailing(key, part):
    base = jnp.clip(jax.random.normal(key, (M, M), jnp.float32), -6.0, 6.0)
    return (base + base.T) * 0.7071


def draw_panel(key, part):
    key_one, key_two, key_three, key_four = jax.random.split(jax.random.fold_in(key, 7), 4)
    base = jnp.clip(jax.random.normal(key_one, (M, B), jnp.float32), -6.0, 6.0)
    shared = jnp.clip(jax.random.normal(key_four, (M,), jnp.float32), -6.0, 6.0)
    magnitude = jax.random.uniform(key_two, (B,), jnp.float32, 6.5, 9.0)
    flips = (2 * jax.random.randint(key_three, (B,), 0, 2) - 1).astype(jnp.float32)
    extra = jnp.concatenate([jnp.diag(flips * magnitude), jnp.zeros((M - B, B), jnp.float32)], axis=0)
    return base + shared[:, None] + extra


def setup_inputs(seed: int = 0) -> dict:
    key_list = jax.random.split(jax.random.key(seed), 3)
    return {
        "trailing": draw_trailing(jax.random.fold_in(key_list[2], 71), 0),
        "panel": draw_panel(jax.random.fold_in(key_list[2], 71), 0),
    }


def matmul(left, right):
    return jnp.dot(left.astype(jnp.float32), right.astype(jnp.float32), precision=lax.Precision.HIGHEST, preferred_element_type=jnp.float32)

def reference(trailing, panel):
    factor_q, factor_r = jnp.linalg.qr(panel)
    flips = jnp.sign(jnp.diagonal(factor_r))
    factor_q = factor_q * flips[None, :]
    factor_r = factor_r * flips[:, None]
    signs = -jnp.sign(jnp.diagonal(factor_q[:B]))
    top_block = factor_q[:B] - jnp.diag(signs)
    reflect = jnp.concatenate([top_block, factor_q[B:]], axis=0)
    block = -signs[:, None] * jnp.linalg.inv(top_block).T
    band = signs[:, None] * factor_r
    products = matmul(trailing, reflect)
    scaled = matmul(products, block)
    inner = matmul(reflect.T, scaled)
    coupling = matmul(block.T, inner)
    weights = scaled - 0.5 * matmul(reflect, coupling)
    left_all = jnp.concatenate([reflect, weights], axis=1)
    right_all = jnp.concatenate([weights, reflect], axis=1)
    pieces = (trailing.reshape(16, M // 16, M), left_all.reshape(16, M // 16, 2 * B))

    def one_block(args):
        rows_part, left_part = args
        return rows_part - matmul(left_part, right_all.T)
    updated = lax.map(one_block, pieces).reshape(M, M)
    return (updated, band)
```

```python
import functools

import jax
import jax.numpy as jnp
from jax import lax
from jax.experimental import pallas as pl
from jax.experimental.pallas import tpu as pltpu
from jax.sharding import Mesh
from jax.sharding import PartitionSpec as P

COL = ("z", "y")
ALL = ("row", "z", "y")
NB = 64
HIGHEST = lax.Precision.HIGHEST
HIGH = lax.Precision.HIGH


def dot(left, right, dims, precision):
    return lax.dot_general(
        left, right, (dims, ((), ())), precision=precision, preferred_element_type=jnp.float32
    )


def nn(left, right, precision=HIGHEST):
    return dot(left, right, ((1,), (0,)), precision)


def nt(left, right, precision=HIGHEST):
    return dot(left, right, ((1,), (1,)), precision)


def tn(left, right, precision=HIGHEST):
    return dot(left, right, ((0,), (0,)), precision)


def unit_eye(n):
    rows = lax.broadcasted_iota(jnp.int32, (n, n), 0)
    cols = lax.broadcasted_iota(jnp.int32, (n, n), 1)
    return (rows == cols).astype(jnp.float32)


def eliminate(block, full):
    aug = jnp.concatenate([block, unit_eye(NB)], axis=1)
    tiles = [aug[8 * i : 8 * i + 8] for i in range(NB // 8)]
    sub = lax.broadcasted_iota(jnp.int32, (8, 1), 0)
    for j in range(NB):
        t, s = divmod(j, 8)
        row = tiles[t][s : s + 1]
        scaled = row * (1.0 / row[:, j : j + 1])
        for i in range(0 if full else t, NB // 8):
            col = tiles[i][:, j : j + 1]
            if i == t:
                if full:
                    new = tiles[i] - jnp.where(sub == s, 0.0, col) * scaled
                    tiles[i] = jnp.where(sub == s, scaled, new)
                else:
                    tiles[i] = tiles[i] - jnp.where(sub > s, col, 0.0) * scaled
            else:
                tiles[i] = tiles[i] - col * scaled
    return jnp.concatenate(tiles, axis=0)


def factor_kernel(gram_ref, top_ref, band_ref, inv_ref, sign_ref, work):
    width = gram_ref.shape[0]
    work[:, :width] = gram_ref[...]
    work[:, width:] = unit_eye(width)
    for k in range(width // NB):
        lo, hi = k * NB, (k + 1) * NB
        done = eliminate(work[lo:hi, lo:hi], False)
        diag = jnp.sum(done[:, :NB] * unit_eye(NB), axis=1, keepdims=True)
        low = done[:, NB:] * lax.rsqrt(diag)
        rows = nn(low, work[lo:hi, :])
        work[lo:hi, :] = rows
        if hi < width:
            work[hi:, :] = work[hi:, :] - tn(rows[:, hi:width], rows)
    eye_r = lax.broadcasted_iota(jnp.int32, (width, width), 0)
    eye_c = lax.broadcasted_iota(jnp.int32, (width, width), 1)
    upper = jnp.where(eye_r <= eye_c, work[:, :width], 0.0)
    inv = jnp.where(eye_r >= eye_c, work[:, width:], 0.0)
    diag_q = jnp.sum(top_ref[...] * inv, axis=1, keepdims=True)
    signs = jnp.where(diag_q > 0.0, -1.0, jnp.where(diag_q < 0.0, 1.0, 0.0))
    band_ref[...] = signs * upper
    inv_ref[...] = inv
    row = jnp.sum(jnp.where(eye_r == eye_c, signs, 0.0), axis=0, keepdims=True)
    sign_ref[...] = jnp.broadcast_to(row, sign_ref.shape)


def block_kernel(top_ref, inv_ref, sign_ref, out_ref, work):
    width = top_ref.shape[0]
    work[:, :width] = unit_eye(width) - nt(inv_ref[...], top_ref[...]) * sign_ref[0:1, :]
    work[:, width:] = unit_eye(width)
    for k in range(width // NB):
        lo, hi = k * NB, (k + 1) * NB
        done = eliminate(work[lo:hi, lo:hi], True)
        rows = nn(done[:, NB:], work[lo:hi, :])
        cols = work[:, lo:hi]
        keep = lax.broadcasted_iota(jnp.int32, (width, 1), 0)
        cols = jnp.where((keep >= lo) & (keep < hi), 0.0, cols)
        work[...] = work[...] - nn(cols, rows)
        work[lo:hi, :] = rows
    out_ref[...] = work[:, width:]


def call(kernel, outs, *args):
    width = args[0].shape[0]
    return pl.pallas_call(
        kernel,
        out_shape=[jax.ShapeDtypeStruct(s, jnp.float32) for s in outs],
        scratch_shapes=[pltpu.VMEM((width, 2 * width), jnp.float32)],
        compiler_params=pltpu.CompilerParams(vmem_limit_bytes=32 * 2**20),
        cost_estimate=pl.CostEstimate(
            flops=2 * 10**9, bytes_accessed=4 * width * width * 6, transcendentals=0
        ),
    )(*args)


def exchange(x, axis):
    return lax.all_to_all(x, axis, 0, 0, tiled=True)


def to_everyone(x, axis):
    return exchange(jnp.broadcast_to(x[None], (lax.axis_size(axis), *x.shape)), axis)


def shift(x, axis, by):
    n = lax.axis_size(axis)
    return lax.ppermute(x, axis, [(i, (i + by) % n) for i in range(n)])


def shards(trailing, panel):
    width = panel.shape[1]
    local_rows = panel.shape[0]
    local_cols = trailing.shape[1]
    rows_n, z_n, y_n = (lax.axis_size(a) for a in ALL)
    row, z, y = (lax.axis_index(a) for a in ALL)
    piece = local_cols // rows_n
    thin = width // rows_n
    first = (row == 0).astype(jnp.float32)

    gram = tn(panel, panel).reshape(rows_n, thin, width)
    top = (first * panel[:width]).reshape(rows_n, thin, width)
    part = jnp.sum(exchange(jnp.concatenate([gram, top], axis=1), "row"), axis=0)
    whole = to_everyone(part, "row")
    gram = whole[:, :thin].reshape(width, width)
    top = whole[:, thin:].reshape(width, width)

    partial = tn(trailing, panel, HIGH).reshape(rows_n, piece, width)
    edge = (first * trailing[:width]).T.reshape(rows_n, piece, width)
    pieces = jnp.sum(exchange(jnp.concatenate([partial, edge], axis=1), "row"), axis=0)
    swap = [
        ((r * z_n + c) * y_n + k, (c * z_n + r) * y_n + k)
        for r in range(rows_n)
        for c in range(z_n)
        for k in range(y_n)
    ]
    mine = lax.dynamic_slice_in_dim(panel, y * local_cols, local_cols, 0)
    panel_piece = lax.ppermute(
        lax.dynamic_slice_in_dim(mine, z * piece, piece, 0), ALL, swap
    )

    band, inv, sign = call(
        factor_kernel, [(width, width), (width, width), (8, width)], gram, top
    )
    (block,) = call(block_kernel, [(width, width)], top, inv, sign)
    sign = sign[0:1]
    diag = unit_eye(width) * sign

    def reflectors(rows_of_panel, is_first, count):
        at = lax.broadcasted_iota(jnp.int32, (count, width), 0)
        to = lax.broadcasted_iota(jnp.int32, (count, width), 1)
        return nt(rows_of_panel, inv, HIGH) - jnp.where(at + is_first == to, sign, 0.0)

    far = 2 * local_rows
    x_piece = nt(pieces[:piece], inv, HIGH) - pieces[piece:] * sign
    y_piece = reflectors(
        panel_piece, jnp.where((z == 0) & (y == 0), row * piece, far), piece
    )
    x_swapped = lax.ppermute(x_piece, ALL, swap)
    x_block = to_everyone(x_swapped, "z").reshape(local_cols, width)
    y_rows = reflectors(panel, jnp.where(row == 0, 0, far), local_rows)
    y_block = lax.dynamic_slice_in_dim(y_rows, y * local_cols, local_cols, 0)

    both = to_everyone(jnp.concatenate([x_piece, y_piece], axis=0), "row")
    x_cols = both[:, :piece].reshape(local_cols, width)
    y_cols = both[:, piece:].reshape(local_cols, width)

    share = width // (rows_n * y_n)
    inner = tn(y_block, x_block).reshape(rows_n * y_n, share, width)
    inner = jnp.sum(exchange(inner, ("row", "y")), axis=0)
    inner = to_everyone(inner, ("row", "y")).reshape(width, width)
    coupling = tn(block, nn(inner, block))

    up = shift(x_block, "y", 1)
    down = shift(x_block, "y", -1)
    half = local_cols // 2
    over = jnp.concatenate([shift(up[:half], "y", 1), shift(down[half:], "y", -1)], axis=0)
    around = jnp.stack([x_block, up, over, down])
    x_rows = jnp.take(around, (y - jnp.arange(y_n)) % y_n, axis=0).reshape(local_rows, width)

    w_cols = nn(x_cols, block, HIGH) - nn(y_cols, coupling, HIGH)
    d_cols = nt(y_cols, block, HIGH)
    left = jnp.concatenate([y_rows, x_rows], axis=1)
    right = jnp.concatenate([w_cols, d_cols], axis=1)
    updated = trailing - nt(left, right, HIGH)
    return (updated, band)


def solution(mesh):
    finer = Mesh(mesh.devices.reshape(mesh.shape["row"], 8, 4), ALL)
    placed = (P("row", COL), P("row", None))
    return jax.shard_map(
        shards, mesh=finer, in_specs=placed, out_specs=(P("row", COL), P()), check_vma=False
    )
```

```python
import functools

import jax
import jax.numpy as jnp
from jax import lax
from jax.experimental import pallas as pl
from jax.experimental.pallas import tpu as pltpu
from jax.sharding import Mesh
from jax.sharding import PartitionSpec as P

ALL = ("x", "core", "z", "y")
NB = 64
WINDOW = 8
STEPS = 4
HIGHEST = lax.Precision.HIGHEST
HIGH = lax.Precision.HIGH


def dot(left, right, dims, precision):
    return lax.dot_general(
        left, right, (dims, ((), ())), precision=precision, preferred_element_type=jnp.float32
    )


def nn(left, right, precision=HIGHEST):
    return dot(left, right, ((1,), (0,)), precision)


def nt(left, right, precision=HIGHEST):
    return dot(left, right, ((1,), (1,)), precision)


def tn(left, right, precision=HIGHEST):
    return dot(left, right, ((0,), (0,)), precision)


def unit_eye(n):
    rows = lax.broadcasted_iota(jnp.int32, (n, n), 0)
    cols = lax.broadcasted_iota(jnp.int32, (n, n), 1)
    return (rows == cols).astype(jnp.float32)


def eliminate(block, full):
    count = NB // 8
    aug = jnp.concatenate([block, unit_eye(NB)], axis=1)
    wide = aug.shape[1]
    tiles = [aug[8 * i : 8 * i + 8] for i in range(count)]
    sub = lax.broadcasted_iota(jnp.int32, (8, wide), 0)

    def spread(j, now):
        first = 0 if full else now // 8
        return {i: jnp.broadcast_to(tiles[i][:, j : j + 1], (8, wide)) for i in range(first, count)}

    def line(tile, s):
        return jnp.broadcast_to(tile[s : s + 1], (8, wide))

    ahead = {j: spread(j, 0) for j in range(min(WINDOW, NB))}
    for j in range(NB):
        t, s = divmod(j, 8)
        mine = ahead.pop(j)
        inverse = 1.0 / line(mine[t], s)
        where = range(0 if full else t, count)
        factor = {i: mine[i] * inverse for i in where}
        factor[t] = jnp.where(sub != s if full else sub > s, factor[t], 0.0)
        scale = jnp.where(sub == s, inverse, 1.0) if full else None

        def step(tile, i, pivot):
            kept = tile * scale if full and i == t else tile
            return kept - factor[i] * pivot

        pivot = line(tiles[t], s)
        for i in where:
            tiles[i] = step(tiles[i], i, pivot)
        for l in sorted(ahead):
            pivot = line(ahead[l][t], s)
            ahead[l] = {i: step(ahead[l][i], i, pivot) for i in ahead[l] if i in where}
        if j + WINDOW < NB:
            ahead[j + WINDOW] = spread(j + WINDOW, j + 1)
    return jnp.concatenate(tiles, axis=0)


def halves(value):
    high = value.astype(jnp.bfloat16)
    return high, (value - high.astype(jnp.float32)).astype(jnp.bfloat16)


def thirds(value):
    high, rest = halves(value)
    low = value - high.astype(jnp.float32) - rest.astype(jnp.float32)
    return high, rest, low.astype(jnp.bfloat16)


def one(left, right, dims):
    return dot(left, right, dims, lax.Precision.DEFAULT)


def dot3(left, right, dims):
    (lh, ll), (rh, rl) = left, right
    (ld,), (rd,) = dims
    return one(jnp.concatenate([lh, lh, ll], axis=ld), jnp.concatenate([rh, rl, rh], axis=rd), dims)


def share_out(core, value, lanes, kept_ref, sent_ref):
    chips, rows, _ = kept_ref.shape
    for q in range(chips):
        for ref, side in ((kept_ref, core), (sent_ref, 1 - core)):
            at = pl.multiple_of((2 * q + side) * rows, rows)
            ref[q, :, lanes] = value[pl.ds(at, rows), :]


def load(refs, buffers, semaphores):
    steps = semaphores.shape[1]

    def copies(c):
        for n, (ref, buffer) in enumerate(zip(refs, buffers)):
            rows = ref.shape[0] // steps
            at = pl.ds(c * rows, rows)
            yield pltpu.make_async_copy(ref.at[at], buffer.at[at], semaphores.at[n, c])

    for c in range(steps):
        for copy in copies(c):
            copy.start()

    def wait(c):
        for copy in copies(c):
            copy.wait()

    return wait


def gram_kernel(place_ref, panel_ref, kept_ref, sent_ref, panel, total, cross, semaphores):
    width = panel.shape[1]
    steps = semaphores.shape[1]
    rows = panel.shape[0] // steps
    wait = load([panel_ref], [panel], semaphores)
    dims = ((1,), (0,))
    for c in range(steps):
        wait(c)
        block = panel[c * rows : (c + 1) * rows]
        high, rest, low = thirds(block)
        high_t, rest_t = halves(block.T)
        same = one(
            jnp.concatenate([high_t, rest_t], axis=1), jnp.concatenate([high, rest], axis=0), dims
        )
        mixed = one(
            jnp.concatenate([high_t, high_t], axis=1), jnp.concatenate([rest, low], axis=0), dims
        )
        total[...] = same if c == 0 else total[...] + same
        cross[...] = mixed if c == 0 else cross[...] + mixed
    total[...] = total[...] + (cross[...] + cross[...].T)
    core = place_ref[1]
    first = (place_ref[0] + core == 0).astype(jnp.float32)
    cross[...] = panel[:width] * first
    share_out(core, total, slice(0, width), kept_ref, sent_ref)
    share_out(core, cross, slice(width, 2 * width), kept_ref, sent_ref)


def product_kernel(
    place_ref, trailing_ref, panel_ref, kept_ref, sent_ref, trailing, panel, total, edge, semaphores
):
    width = panel.shape[1]
    steps = semaphores.shape[1]
    rows = panel.shape[0] // steps
    wait = load([trailing_ref, panel_ref], [trailing, panel], semaphores)
    core = place_ref[1]
    first = (place_ref[0] + core == 0).astype(jnp.float32)
    for c in range(steps):
        wait(c)
        at = slice(c * rows, (c + 1) * rows)
        tile_t = trailing[at].T
        if c == 0:
            edge[...] = tile_t[:, :width] * first
        part = dot3(halves(tile_t), halves(panel[at]), ((1,), (0,)))
        total[...] = part if c == 0 else total[...] + part
    share_out(core, total, slice(0, width), kept_ref, sent_ref)
    share_out(core, edge, slice(width, 2 * width), kept_ref, sent_ref)


def stream_call(kernel, place, arrays, out, scratch, flops):
    return pl.pallas_call(
        kernel,
        out_shape=[jax.ShapeDtypeStruct(out, jnp.float32)] * 2,
        in_specs=[pl.BlockSpec(memory_space=pltpu.SMEM)]
        + [pl.BlockSpec(memory_space=pltpu.HBM)] * len(arrays),
        out_specs=[pl.BlockSpec(memory_space=pltpu.VMEM)] * 2,
        scratch_shapes=[pltpu.VMEM(a.shape, jnp.float32) for a in arrays]
        + [pltpu.VMEM(s, jnp.float32) for s in scratch]
        + [pltpu.SemaphoreType.DMA((len(arrays), STEPS))],
        compiler_params=pltpu.CompilerParams(vmem_limit_bytes=65_500_000),
        cost_estimate=estimate(flops),
    )(place, *arrays)


def factor_kernel(place_ref, sums_ref, other_ref, band_ref, inv_ref, sign_ref, top_ref, work, whole):
    width = band_ref.shape[0]
    ring, thin, _ = sums_ref.shape
    x, core = place_ref[0], place_ref[1]
    for s in range(ring):
        base = lax.rem(x + ring - s, ring) * (2 * thin)
        whole[pl.ds(pl.multiple_of(base + core * thin, thin), thin), :] = sums_ref[s]
        whole[pl.ds(pl.multiple_of(base + (1 - core) * thin, thin), thin), :] = other_ref[s]
    work[:, :width] = whole[:, :width]
    work[:, width:] = unit_eye(width)
    top_ref[...] = whole[:, width:]
    for k in range(width // NB):
        lo, hi = k * NB, (k + 1) * NB
        done = eliminate(work[lo:hi, lo:hi], False)
        diag = jnp.sum(done[:, :NB] * unit_eye(NB), axis=1, keepdims=True)
        low = done[:, NB:] * lax.rsqrt(diag)
        rows = nn(low, work[lo:hi, :])
        work[lo:hi, :] = rows
        if hi < width:
            work[hi:, :] = work[hi:, :] - tn(rows[:, hi:width], rows)
    eye_r = lax.broadcasted_iota(jnp.int32, (width, width), 0)
    eye_c = lax.broadcasted_iota(jnp.int32, (width, width), 1)
    upper = jnp.where(eye_r <= eye_c, work[:, :width], 0.0)
    inv = jnp.where(eye_r >= eye_c, work[:, width:], 0.0)
    diag_q = jnp.sum(top_ref[...] * inv, axis=1, keepdims=True)
    signs = jnp.where(diag_q > 0.0, -1.0, jnp.where(diag_q < 0.0, 1.0, 0.0))
    band_ref[...] = signs * upper
    inv_ref[...] = inv
    row = jnp.sum(jnp.where(eye_r == eye_c, signs, 0.0), axis=0, keepdims=True)
    sign_ref[...] = jnp.broadcast_to(row, sign_ref.shape)


def block_kernel(top_ref, inv_ref, sign_ref, out_ref, work):
    width = top_ref.shape[0]
    work[:, :width] = unit_eye(width) - nt(inv_ref[...], top_ref[...]) * sign_ref[0:1, :]
    work[:, width:] = unit_eye(width)
    for k in range(width // NB):
        lo, hi = k * NB, (k + 1) * NB
        done = eliminate(work[lo:hi, lo:hi], True)
        rows = nn(done[:, NB:], work[lo:hi, :])
        cols = work[:, lo:hi]
        keep = lax.broadcasted_iota(jnp.int32, (width, 1), 0)
        cols = jnp.where((keep >= lo) & (keep < hi), 0.0, cols)
        work[...] = work[...] - nn(cols, rows)
        work[lo:hi, :] = rows
    out_ref[...] = work[:, width:]


def update_kernel(
    place_ref, trailing_ref, y_ref, own_ref, up_ref, over_ref, down_ref, cols_ref, other_ref,
    block_ref, coupling_ref, out_ref, tile, result, whole, right, left, semaphores, done,
):
    width = block_ref.shape[0]
    count = own_ref.shape[0]
    sources = (own_ref, up_ref, over_ref, down_ref)

    def rows_of(step):
        to = lax.rem(place_ref[2] + len(sources) - step, len(sources))
        return pl.ds(pl.multiple_of(to * count, count), count)

    def loading(step):
        return pltpu.make_async_copy(
            trailing_ref.at[rows_of(step)], tile.at[step], semaphores.at[step]
        )

    def storing(step):
        return pltpu.make_async_copy(result.at[step], out_ref.at[rows_of(step)], done.at[step])

    for step in range(len(sources)):
        loading(step).start()
    ring, piece, _ = cols_ref.shape
    x, core = place_ref[0], place_ref[1]
    for s in range(ring):
        base = lax.rem(x + ring - s, ring) * (2 * piece)
        whole[pl.ds(pl.multiple_of(base + core * piece, piece), piece), :] = cols_ref[s]
        whole[pl.ds(pl.multiple_of(base + (1 - core) * piece, piece), piece), :] = other_ref[s]
    block = halves(block_ref[...])
    x_cols, y_cols = halves(whole[:, :width]), halves(whole[:, width:])
    w = dot3(x_cols, block, ((1,), (0,)))
    w = w - dot3(y_cols, halves(coupling_ref[...]), ((1,), (0,)))
    d = dot3(y_cols, block, ((1,), (1,)))
    high, low = halves(jnp.concatenate([w, d], axis=1).T)
    span = high.shape[0]
    right[:span] = high
    right[span : 2 * span] = low
    right[2 * span :] = high
    for step, ref in enumerate(sources):
        high, low = halves(ref[...])
        left[:, width : 2 * width] = high
        left[:, 3 * width : 4 * width] = high
        left[:, 5 * width :] = low
        high, low = halves(y_ref[rows_of(step), :])
        left[:, :width] = high
        left[:, 2 * width : 3 * width] = high
        left[:, 4 * width : 5 * width] = low
        loading(step).wait()
        result[step] = tile[step] - one(left[...], right[...], ((1,), (0,)))
        storing(step).start()
    for step in range(len(sources)):
        storing(step).wait()


def local_call(kernel, outs, scratch, *args, **more):
    return pl.pallas_call(
        kernel,
        out_shape=[jax.ShapeDtypeStruct(s, jnp.float32) for s in outs],
        scratch_shapes=[pltpu.VMEM(s, t) for s, t in scratch],
        compiler_params=pltpu.CompilerParams(vmem_limit_bytes=40 * 2**20),
        **more,
    )(*args)


def estimate(flops):
    return pl.CostEstimate(flops=flops, bytes_accessed=2**20, transcendentals=0)


def update_call(place, trailing, y_rows, sources, cols, cols_other, block, coupling):
    count, width = sources[0].shape
    y_n = len(sources)
    tiles = (y_n, count, trailing.shape[1])
    args = (y_rows, *sources, cols, cols_other, block, coupling)
    return pl.pallas_call(
        update_kernel,
        name="update_kernel",
        out_shape=jax.ShapeDtypeStruct(trailing.shape, jnp.float32),
        in_specs=[pl.BlockSpec(memory_space=pltpu.SMEM), pl.BlockSpec(memory_space=pltpu.HBM)]
        + [pl.BlockSpec(memory_space=pltpu.VMEM)] * len(args),
        out_specs=pl.BlockSpec(memory_space=pltpu.HBM),
        scratch_shapes=[
            pltpu.VMEM(tiles, jnp.float32),
            pltpu.VMEM(tiles, jnp.float32),
            pltpu.VMEM((trailing.shape[1], 2 * width), jnp.float32),
            pltpu.VMEM((6 * width, trailing.shape[1]), jnp.bfloat16),
            pltpu.VMEM((count, 6 * width), jnp.bfloat16),
            pltpu.SemaphoreType.DMA((y_n,)),
            pltpu.SemaphoreType.DMA((y_n,)),
        ],
        compiler_params=pltpu.CompilerParams(vmem_limit_bytes=56 * 2**20),
        cost_estimate=estimate(2 * 10**9),
    )(place, trailing, *args)


def exchange(x, axis):
    return lax.all_to_all(x, axis, 0, 0, tiled=True)


def to_everyone(x, axis):
    return exchange(jnp.broadcast_to(x[None], (lax.axis_size(axis), *x.shape)), axis)


def shift(x, axis, by):
    n = lax.axis_size(axis)
    return lax.ppermute(x, axis, [(i, (i + by) % n) for i in range(n)])


def around(x, axis):
    found = [x]
    for s in range(1, lax.axis_size(axis)):
        found.append(shift(x, axis, s))
    return found


def scatter_sum(parts, axis):
    n = lax.axis_size(axis)
    me = lax.axis_index(axis)
    total = lax.dynamic_index_in_dim(parts, me, 0, keepdims=False)
    for s in range(1, n):
        to = lax.dynamic_index_in_dim(parts, (me + s) % n, 0, keepdims=False)
        total = total + shift(to, axis, s)
    return total


def pair_sum(kept, sent):
    return kept + shift(sent, "core", 1)


def shards(trailing, panel):
    width = panel.shape[1]
    local_rows = panel.shape[0]
    local_cols = trailing.shape[1]
    x_n, core_n, z_n, y_n = (lax.axis_size(a) for a in ALL)
    x, core, z, y = (lax.axis_index(a) for a in ALL)
    row = x * core_n + core
    rows_n = x_n * core_n
    piece = local_cols // rows_n
    thin = width // rows_n
    first = (row == 0).astype(jnp.float32)
    swap = [
        ((r * z_n + c) * y_n + k, (c * z_n + r) * y_n + k)
        for r in range(rows_n)
        for c in range(z_n)
        for k in range(y_n)
    ]
    place = jnp.stack([x, core, y]).astype(jnp.int32)

    kept, sent = stream_call(
        product_kernel,
        place,
        [trailing, panel],
        (x_n, piece, 2 * width),
        [(local_cols, width)] * 2,
        2 * 10**9,
    )
    pieces = scatter_sum(pair_sum(kept, sent), "x")

    kept, sent = stream_call(
        gram_kernel, place, [panel], (x_n, thin, 2 * width), [(width, width)] * 2, 10**9
    )
    sums = jnp.stack(around(scatter_sum(pair_sum(kept, sent), "x"), "x"))
    other = shift(sums, "core", 1)

    mine = lax.dynamic_slice_in_dim(panel, y * local_cols, local_cols, 0)
    to_swap = lax.dynamic_slice_in_dim(mine, z * piece, piece, 0)
    swapped = lax.ppermute(jnp.concatenate([pieces, to_swap], axis=1), ALL, swap)
    panel_piece = swapped[:, 2 * width :]

    smem = pl.BlockSpec(memory_space=pltpu.SMEM)
    vmem = pl.BlockSpec(memory_space=pltpu.VMEM)
    band, inv, sign, top = local_call(
        factor_kernel,
        [(width, width), (width, width), (8, width), (width, width)],
        [((width, 2 * width), jnp.float32)] * 2,
        place, sums, other,
        in_specs=[smem, vmem, vmem],
        cost_estimate=estimate(3 * 10**9),
    )
    (block,) = local_call(
        block_kernel,
        [(width, width)],
        [((width, 2 * width), jnp.float32)],
        top, inv, sign,
        cost_estimate=estimate(4 * 10**9),
    )
    sign = sign[0:1]

    def reflectors(rows_of_panel, is_first, count):
        at = lax.broadcasted_iota(jnp.int32, (count, width), 0)
        to = lax.broadcasted_iota(jnp.int32, (count, width), 1)
        return nt(rows_of_panel, inv, HIGH) - jnp.where(at + is_first == to, sign, 0.0)

    far = 2 * local_rows

    def products(both):
        return nt(both[:, :width], inv, HIGH) - both[:, width : 2 * width] * sign

    x_block = to_everyone(products(swapped), "z").reshape(local_cols, width)
    y_block = reflectors(mine, jnp.where(row == 0, y * local_cols, far), local_cols)
    y_rows = reflectors(panel, jnp.where(row == 0, 0, far), local_rows)
    y_piece = reflectors(
        panel_piece, jnp.where((z == 0) & (y == 0), row * piece, far), piece
    )
    cols = jnp.stack(around(jnp.concatenate([products(pieces), y_piece], axis=1), "x"))
    cols_other = shift(cols, "core", 1)

    x_block, block = lax.optimization_barrier((x_block, block))
    inner = tn(y_block, x_block)
    inner = lax.dynamic_slice_in_dim(inner, z * (width // z_n), width // z_n, 0)
    inner, x_block = lax.optimization_barrier((inner, x_block))
    for axis in ("y", "core", "x"):
        inner = functools.reduce(jnp.add, around(inner, axis))
    inner = to_everyone(inner, "z").reshape(width, width)
    coupling = tn(block, nn(inner, block))
    sources = around(x_block, "y")

    updated = update_call(place, trailing, y_rows, sources, cols, cols_other, block, coupling)
    return (updated, band)


def solution(mesh):
    finer = Mesh(mesh.devices.reshape(mesh.shape["row"] // 2, 2, 8, 4), ALL)
    placed = (P(("x", "core"), ("z", "y")), P(("x", "core"), None))
    return jax.shard_map(
        shards,
        mesh=finer,
        in_specs=placed,
        out_specs=(P(("x", "core"), ("z", "y")), P()),
        check_vma=False,
    )
```

```python
import functools

import jax
import jax.numpy as jnp
from jax import lax
from jax.experimental import pallas as pl
from jax.experimental.pallas import tpu as pltpu
from jax.sharding import Mesh
from jax.sharding import PartitionSpec as P

ALL = ("x", "core", "z", "y")
NB = 64
WINDOW = 8
WINDOW_FULL = 6
STEPS = 4
HIGHEST = lax.Precision.HIGHEST
HIGH = lax.Precision.HIGH


def dot(left, right, dims, precision):
    return lax.dot_general(
        left, right, (dims, ((), ())), precision=precision, preferred_element_type=jnp.float32
    )


def nn(left, right, precision=HIGHEST):
    return dot(left, right, ((1,), (0,)), precision)


def nt(left, right, precision=HIGHEST):
    return dot(left, right, ((1,), (1,)), precision)


def tn(left, right, precision=HIGHEST):
    return dot(left, right, ((0,), (0,)), precision)


def unit_eye(n):
    rows = lax.broadcasted_iota(jnp.int32, (n, n), 0)
    cols = lax.broadcasted_iota(jnp.int32, (n, n), 1)
    return (rows == cols).astype(jnp.float32)


def at_block(k, value, size):
    found = value[:, :size]
    for j in range(1, value.shape[1] // size):
        found = jnp.where(k == j, value[:, j * size : (j + 1) * size], found)
    return found


def eliminate(block, full):
    count = NB // 8
    window = WINDOW_FULL if full else WINDOW
    aug = jnp.concatenate([block, unit_eye(NB)], axis=1)
    wide = aug.shape[1]
    tiles = [aug[8 * i : 8 * i + 8] for i in range(count)]
    sub = lax.broadcasted_iota(jnp.int32, (8, wide), 0)

    def spread(j, now):
        first = 0 if full else now // 8
        return {i: jnp.broadcast_to(tiles[i][:, j : j + 1], (8, wide)) for i in range(first, count)}

    def line(tile, s):
        return jnp.broadcast_to(tile[s : s + 1], (8, wide))

    ahead = {j: spread(j, 0) for j in range(min(window, NB))}
    for j in range(NB):
        t, s = divmod(j, 8)
        mine = ahead.pop(j)
        inverse = 1.0 / line(mine[t], s)
        where = range(0 if full else t, count)
        factor = {i: mine[i] * inverse for i in where}
        factor[t] = jnp.where(sub != s if full else sub > s, factor[t], 0.0)
        scale = jnp.where(sub == s, inverse, 1.0) if full else None

        def step(tile, i, pivot):
            kept = tile * scale if full and i == t else tile
            return kept - factor[i] * pivot

        pivot = line(tiles[t], s)
        for i in where:
            tiles[i] = step(tiles[i], i, pivot)
        for l in sorted(ahead):
            pivot = line(ahead[l][t], s)
            ahead[l] = {i: step(ahead[l][i], i, pivot) for i in ahead[l] if i in where}
        if j + window < NB:
            ahead[j + window] = spread(j + window, j + 1)
    return jnp.concatenate(tiles, axis=0)


def halves(value):
    high = value.astype(jnp.bfloat16)
    return high, (value - high.astype(jnp.float32)).astype(jnp.bfloat16)


def thirds(value):
    high, rest = halves(value)
    low = value - high.astype(jnp.float32) - rest.astype(jnp.float32)
    return high, rest, low.astype(jnp.bfloat16)


def one(left, right, dims):
    return dot(left, right, dims, lax.Precision.DEFAULT)


def dot3(left, right, dims):
    (lh, ll), (rh, rl) = left, right
    (ld,), (rd,) = dims
    return one(jnp.concatenate([lh, lh, ll], axis=ld), jnp.concatenate([rh, rl, rh], axis=rd), dims)


def share_out(core, value, lanes, kept_ref, sent_ref):
    chips, rows, _ = kept_ref.shape
    for q in range(chips):
        for ref, side in ((kept_ref, core), (sent_ref, 1 - core)):
            at = pl.multiple_of((2 * q + side) * rows, rows)
            ref[q, :, lanes] = value[pl.ds(at, rows), :]


def gram_kernel(place_ref, panel_ref, kept_ref, sent_ref, total, cross):
    width = panel_ref.shape[1]
    rows = panel_ref.shape[0] // STEPS
    dims = ((1,), (0,))
    total[...] = jnp.zeros_like(total)
    cross[...] = jnp.zeros_like(cross)

    @pl.loop(0, STEPS)
    def _(c):
        block = panel_ref[pl.ds(pl.multiple_of(c * rows, rows), rows), :]
        high, rest, low = thirds(block)
        high_t, rest_t = halves(block.T)
        total[...] += one(
            jnp.concatenate([high_t, rest_t], axis=1), jnp.concatenate([high, rest], axis=0), dims
        )
        cross[...] += one(
            jnp.concatenate([high_t, high_t], axis=1), jnp.concatenate([rest, low], axis=0), dims
        )

    total[...] = total[...] + (cross[...] + cross[...].T)
    core = place_ref[1]
    first = (place_ref[0] + core == 0).astype(jnp.float32)
    cross[...] = panel_ref[:width] * first
    share_out(core, total, slice(0, width), kept_ref, sent_ref)
    share_out(core, cross, slice(width, 2 * width), kept_ref, sent_ref)


def product_kernel(place_ref, trailing_ref, panel_ref, kept_ref, sent_ref, total, edge):
    width = panel_ref.shape[1]
    rows = panel_ref.shape[0] // STEPS
    core = place_ref[1]
    first = (place_ref[0] + core == 0).astype(jnp.float32)
    edge[...] = trailing_ref[:width].T * first
    total[...] = jnp.zeros_like(total)

    @pl.loop(0, STEPS)
    def _(c):
        at = pl.ds(pl.multiple_of(c * rows, rows), rows)
        total[...] += dot3(halves(trailing_ref[at, :].T), halves(panel_ref[at, :]), ((1,), (0,)))

    share_out(core, total, slice(0, width), kept_ref, sent_ref)
    share_out(core, edge, slice(width, 2 * width), kept_ref, sent_ref)


def stream_call(kernel, place, arrays, out, scratch, flops):
    vmem = pl.BlockSpec(memory_space=pltpu.VMEM)
    return pl.pallas_call(
        kernel,
        out_shape=[jax.ShapeDtypeStruct(out, jnp.float32)] * 2,
        in_specs=[pl.BlockSpec(memory_space=pltpu.SMEM)] + [vmem] * len(arrays),
        out_specs=[vmem] * 2,
        scratch_shapes=[pltpu.VMEM(s, jnp.float32) for s in scratch],
        compiler_params=pltpu.CompilerParams(vmem_limit_bytes=24 * 2**20),
        cost_estimate=estimate(flops),
    )(place, *arrays)


def factor_kernel(place_ref, sums_ref, other_ref, band_ref, inv_ref, sign_ref, top_ref, work, whole):
    width = band_ref.shape[0]
    ring, thin, _ = sums_ref.shape
    x, core = place_ref[0], place_ref[1]
    for s in range(ring):
        base = lax.rem(x + ring - s, ring) * (2 * thin)
        whole[pl.ds(pl.multiple_of(base + core * thin, thin), thin), :] = sums_ref[s]
        whole[pl.ds(pl.multiple_of(base + (1 - core) * thin, thin), thin), :] = other_ref[s]
    work[:, :width] = whole[:, :width]
    work[:, width:] = unit_eye(width)
    top_ref[...] = whole[:, width:]
    for k in range(width // NB):
        lo, hi = k * NB, (k + 1) * NB
        done = eliminate(work[lo:hi, lo:hi], False)
        diag = jnp.sum(done[:, :NB] * unit_eye(NB), axis=1, keepdims=True)
        low = done[:, NB:] * lax.rsqrt(diag)
        right = width + hi
        rows = nn(low, work[lo:hi, lo:right])
        work[lo:hi, lo:right] = rows
        if hi < width:
            work[hi:, hi:right] = work[hi:, hi:right] - tn(rows[:, NB : width - lo], rows[:, NB:])

    eye_r = lax.broadcasted_iota(jnp.int32, (width, width), 0)
    eye_c = lax.broadcasted_iota(jnp.int32, (width, width), 1)
    upper = jnp.where(eye_r <= eye_c, work[:, :width], 0.0)
    inv = jnp.where(eye_r >= eye_c, work[:, width:], 0.0)
    diag_q = jnp.sum(top_ref[...] * inv, axis=1, keepdims=True)
    signs = jnp.where(diag_q > 0.0, -1.0, jnp.where(diag_q < 0.0, 1.0, 0.0))
    band_ref[...] = signs * upper
    inv_ref[...] = inv
    row = jnp.sum(jnp.where(eye_r == eye_c, signs, 0.0), axis=0, keepdims=True)
    sign_ref[...] = jnp.broadcast_to(row, sign_ref.shape)


def block_kernel(top_ref, inv_ref, sign_ref, out_ref, work, side):
    width = top_ref.shape[0]
    work[:, :width] = unit_eye(width) - nt(inv_ref[...], top_ref[...]) * sign_ref[0:1, :]
    work[:, width:] = unit_eye(width)
    index = lax.broadcasted_iota(jnp.int32, (width, 1), 0)

    @pl.loop(0, width // NB)
    def _(k):
        lo = pl.multiple_of(k * NB, NB)
        cols = at_block(k, work[:, :width], NB)
        side[...] = cols
        done = eliminate(side[pl.ds(lo, NB), :], True)
        rows = nn(done[:, NB:], work[pl.ds(lo, NB), :])
        cols = jnp.where((index >= lo) & (index < lo + NB), 0.0, cols)
        work[...] = work[...] - dot3(halves(cols), halves(rows), ((1,), (0,)))
        work[pl.ds(lo, NB), :] = rows

    out_ref[...] = work[:, width:]


def right_kernel(
    place_ref, cols_ref, other_ref, block_ref, coupling_ref, right_ref, whole
):
    width = block_ref.shape[0]
    ring, piece, _ = cols_ref.shape
    x, core = place_ref[0], place_ref[1]
    for s in range(ring):
        base = lax.rem(x + ring - s, ring) * (2 * piece)
        whole[pl.ds(pl.multiple_of(base + core * piece, piece), piece), :] = cols_ref[s]
        whole[pl.ds(pl.multiple_of(base + (1 - core) * piece, piece), piece), :] = other_ref[s]
    block = halves(block_ref[...])
    x_cols, y_cols = halves(whole[:, :width]), halves(whole[:, width:])
    w = dot3(x_cols, block, ((1,), (0,)))
    w = w - dot3(y_cols, halves(coupling_ref[...]), ((1,), (0,)))
    d = dot3(y_cols, block, ((1,), (1,)))
    high, low = halves(jnp.concatenate([w, d], axis=1).T)
    span = high.shape[0]
    right_ref[:span] = high
    right_ref[span : 2 * span] = low
    right_ref[2 * span :] = high


def update_kernel(
    place_ref, trailing_ref, y_ref, own_ref, up_ref, over_ref, down_ref, right_ref,
    out_ref, tile, result, left, semaphores, done,
):
    count, width = own_ref.shape
    sources = (own_ref, up_ref, over_ref, down_ref)

    def rows_of(step):
        to = lax.rem(place_ref[2] + len(sources) - step, len(sources))
        return pl.ds(pl.multiple_of(to * count, count), count)

    def loading(step):
        return pltpu.make_async_copy(
            trailing_ref.at[rows_of(step)], tile.at[step], semaphores.at[step]
        )

    def storing(step):
        return pltpu.make_async_copy(result.at[step], out_ref.at[rows_of(step)], done.at[step])

    for step in range(len(sources)):
        loading(step).start()

    @pl.loop(0, len(sources))
    def _(step):
        for n, source in enumerate(sources):

            @pl.when(step == n)
            def _():
                high, low = halves(source[...])
                left[:, width : 2 * width] = high
                left[:, 3 * width : 4 * width] = high
                left[:, 5 * width :] = low

        high, low = halves(y_ref[rows_of(step), :])
        left[:, :width] = high
        left[:, 2 * width : 3 * width] = high
        left[:, 4 * width : 5 * width] = low
        loading(step).wait()
        result[step] = tile[step] - one(left[...], right_ref[...], ((1,), (0,)))
        storing(step).start()

    for step in range(len(sources)):
        storing(step).wait()


def local_call(kernel, outs, scratch, *args, **more):
    return pl.pallas_call(
        kernel,
        out_shape=[jax.ShapeDtypeStruct(s, jnp.float32) for s in outs],
        scratch_shapes=[pltpu.VMEM(s, t) for s, t in scratch],
        compiler_params=pltpu.CompilerParams(vmem_limit_bytes=30 * 2**20),
        **more,
    )(*args)


def estimate(flops):
    return pl.CostEstimate(flops=flops, bytes_accessed=2**20, transcendentals=0)


def update_call(place, trailing, y_rows, sources, cols, cols_other, block, coupling):
    count, width = sources[0].shape
    y_n = len(sources)
    span = trailing.shape[1]
    tiles = (y_n, count, span)
    smem = pl.BlockSpec(memory_space=pltpu.SMEM)
    vmem = pl.BlockSpec(memory_space=pltpu.VMEM)
    hbm = pl.BlockSpec(memory_space=pltpu.HBM)
    right = pl.pallas_call(
        right_kernel,
        name="right_kernel",
        out_shape=jax.ShapeDtypeStruct((6 * width, span), jnp.bfloat16),
        in_specs=[smem] + [vmem] * 4,
        out_specs=vmem,
        scratch_shapes=[pltpu.VMEM((span, 2 * width), jnp.float32)],
        compiler_params=pltpu.CompilerParams(vmem_limit_bytes=30 * 2**20),
        cost_estimate=estimate(2 * 10**9),
    )(place, cols, cols_other, block, coupling)
    args = (y_rows, *sources, right)
    return pl.pallas_call(
        update_kernel,
        name="update_kernel",
        out_shape=jax.ShapeDtypeStruct(trailing.shape, jnp.float32),
        in_specs=[smem, hbm] + [vmem] * len(args),
        out_specs=hbm,
        scratch_shapes=[
            pltpu.VMEM(tiles, jnp.float32),
            pltpu.VMEM(tiles, jnp.float32),
            pltpu.VMEM((count, 6 * width), jnp.bfloat16),
            pltpu.SemaphoreType.DMA((y_n,)),
            pltpu.SemaphoreType.DMA((y_n,)),
        ],
        compiler_params=pltpu.CompilerParams(vmem_limit_bytes=30 * 2**20),
        cost_estimate=estimate(2 * 10**9),
    )(place, trailing, *args)


def exchange(x, axis):
    return lax.all_to_all(x, axis, 0, 0, tiled=True)


def to_everyone(x, axis):
    return exchange(jnp.broadcast_to(x[None], (lax.axis_size(axis), *x.shape)), axis)


def shift(x, axis, by):
    n = lax.axis_size(axis)
    return lax.ppermute(x, axis, [(i, (i + by) % n) for i in range(n)])


def around(x, axis):
    found = [x]
    for s in range(1, lax.axis_size(axis)):
        found.append(shift(x, axis, s))
    return found


def scatter_sum(parts, axis):
    n = lax.axis_size(axis)
    me = lax.axis_index(axis)
    total = lax.dynamic_index_in_dim(parts, me, 0, keepdims=False)
    for s in range(1, n):
        to = lax.dynamic_index_in_dim(parts, (me + s) % n, 0, keepdims=False)
        total = total + shift(to, axis, s)
    return total


def pair_sum(kept, sent):
    return kept + shift(sent, "core", 1)


def shards(trailing, panel):
    width = panel.shape[1]
    local_rows = panel.shape[0]
    local_cols = trailing.shape[1]
    x_n, core_n, z_n, y_n = (lax.axis_size(a) for a in ALL)
    x, core, z, y = (lax.axis_index(a) for a in ALL)
    row = x * core_n + core
    rows_n = x_n * core_n
    piece = local_cols // rows_n
    thin = width // rows_n
    first = (row == 0).astype(jnp.float32)
    swap = [
        ((r * z_n + c) * y_n + k, (c * z_n + r) * y_n + k)
        for r in range(rows_n)
        for c in range(z_n)
        for k in range(y_n)
    ]
    place = jnp.stack([x, core, y]).astype(jnp.int32)

    kept, sent = stream_call(
        gram_kernel,
        place,
        [panel],
        (x_n, thin, 2 * width),
        [(width, width)] * 2,
        10**9,
    )
    sums = jnp.stack(around(scatter_sum(pair_sum(kept, sent), "x"), "x"))
    other = shift(sums, "core", 1)

    kept, sent = stream_call(
        product_kernel,
        place,
        [trailing, panel],
        (x_n, piece, 2 * width),
        [(local_cols, width)] * 2,
        2 * 10**9,
    )
    pieces = scatter_sum(pair_sum(kept, sent), "x")
    mine = lax.dynamic_slice_in_dim(panel, y * local_cols, local_cols, 0)
    to_swap = lax.dynamic_slice_in_dim(panel, y * local_cols + z * piece, piece, 0)
    swapped = lax.ppermute(jnp.concatenate([pieces, to_swap], axis=1), ALL, swap)
    panel_piece = swapped[:, 2 * width :]

    smem = pl.BlockSpec(memory_space=pltpu.SMEM)
    vmem = pl.BlockSpec(memory_space=pltpu.VMEM)
    band, inv, sign, top = local_call(
        factor_kernel,
        [(width, width), (width, width), (8, width), (width, width)],
        [((width, 2 * width), jnp.float32)] * 2,
        place, sums, other,
        in_specs=[smem, vmem, vmem],
        cost_estimate=estimate(3 * 10**9),
    )
    (block,) = local_call(
        block_kernel,
        [(width, width)],
        [((width, 2 * width), jnp.float32), ((width, NB), jnp.float32)],
        top, inv, sign,
        cost_estimate=estimate(4 * 10**9),
    )
    sign = sign[0:1]

    def reflectors(rows_of_panel, is_first, count):
        at = lax.broadcasted_iota(jnp.int32, (count, width), 0)
        to = lax.broadcasted_iota(jnp.int32, (count, width), 1)
        return nt(rows_of_panel, inv, HIGH) - jnp.where(at + is_first == to, sign, 0.0)

    far = 2 * local_rows

    def products(both):
        return nt(both[:, :width], inv, HIGH) - both[:, width : 2 * width] * sign

    x_block = to_everyone(products(swapped), "z").reshape(local_cols, width)
    y_block = reflectors(mine, jnp.where(row == 0, y * local_cols, far), local_cols)
    y_rows = reflectors(panel, jnp.where(row == 0, 0, far), local_rows)
    y_piece = reflectors(
        panel_piece, jnp.where((z == 0) & (y == 0), row * piece, far), piece
    )
    cols = jnp.stack(around(jnp.concatenate([products(pieces), y_piece], axis=1), "x"))
    cols_other = shift(cols, "core", 1)

    x_block, block = lax.optimization_barrier((x_block, block))
    inner = tn(y_block, x_block)
    inner = lax.dynamic_slice_in_dim(inner, z * (width // z_n), width // z_n, 0)
    inner, x_block = lax.optimization_barrier((inner, x_block))
    for axis in ("y", "core", "x"):
        inner = functools.reduce(jnp.add, around(inner, axis))
    inner = to_everyone(inner, "z").reshape(width, width)
    coupling = tn(block, nn(inner, block))
    sources = around(x_block, "y")

    updated = update_call(place, trailing, y_rows, sources, cols, cols_other, block, coupling)
    return (updated, band)


def solution(mesh):
    finer = Mesh(mesh.devices.reshape(mesh.shape["row"] // 2, 2, 8, 4), ALL)
    placed = (P(("x", "core"), ("z", "y")), P(("x", "core"), None))
    return jax.shard_map(
        shards,
        mesh=finer,
        in_specs=placed,
        out_specs=(P(("x", "core"), ("z", "y")), P()),
        check_vma=False,
    )
```

```python
import functools

import jax
import jax.numpy as jnp
from jax import lax
from jax.experimental import pallas as pl
from jax.experimental.pallas import tpu as pltpu
from jax.sharding import Mesh
from jax.sharding import PartitionSpec as P

ALL = ("x", "core", "z", "y")
NB = 64
WINDOW = 8
WINDOW_FULL = 6
STEPS = 4
HIGHEST = lax.Precision.HIGHEST
HIGH = lax.Precision.HIGH


def dot(left, right, dims, precision):
    return lax.dot_general(
        left, right, (dims, ((), ())), precision=precision, preferred_element_type=jnp.float32
    )


def nn(left, right, precision=HIGHEST):
    return dot(left, right, ((1,), (0,)), precision)


def nt(left, right, precision=HIGHEST):
    return dot(left, right, ((1,), (1,)), precision)


def tn(left, right, precision=HIGHEST):
    return dot(left, right, ((0,), (0,)), precision)


def unit_eye(n):
    rows = lax.broadcasted_iota(jnp.int32, (n, n), 0)
    cols = lax.broadcasted_iota(jnp.int32, (n, n), 1)
    return (rows == cols).astype(jnp.float32)


def at_block(k, value, size):
    found = value[:, :size]
    for j in range(1, value.shape[1] // size):
        found = jnp.where(k == j, value[:, j * size : (j + 1) * size], found)
    return found


def eliminate(block, full):
    count = NB // 8
    window = WINDOW_FULL if full else WINDOW
    aug = jnp.concatenate([block, unit_eye(NB)], axis=1)
    wide = aug.shape[1]
    tiles = [aug[8 * i : 8 * i + 8] for i in range(count)]
    sub = lax.broadcasted_iota(jnp.int32, (8, wide), 0)

    def spread(j, now):
        first = 0 if full else now // 8
        return {i: jnp.broadcast_to(tiles[i][:, j : j + 1], (8, wide)) for i in range(first, count)}

    def line(tile, s):
        return jnp.broadcast_to(tile[s : s + 1], (8, wide))

    ahead = {j: spread(j, 0) for j in range(min(window, NB))}
    for j in range(NB):
        t, s = divmod(j, 8)
        mine = ahead.pop(j)
        inverse = 1.0 / line(mine[t], s)
        where = range(0 if full else t, count)
        factor = {i: mine[i] * inverse for i in where}
        factor[t] = jnp.where(sub != s if full else sub > s, factor[t], 0.0)
        scale = jnp.where(sub == s, inverse, 1.0) if full else None

        def step(tile, i, pivot):
            kept = tile * scale if full and i == t else tile
            return kept - factor[i] * pivot

        pivot = line(tiles[t], s)
        for i in where:
            tiles[i] = step(tiles[i], i, pivot)
        for l in sorted(ahead):
            pivot = line(ahead[l][t], s)
            ahead[l] = {i: step(ahead[l][i], i, pivot) for i in ahead[l] if i in where}
        if j + window < NB:
            ahead[j + window] = spread(j + window, j + 1)
    return jnp.concatenate(tiles, axis=0)


def halves(value):
    high = value.astype(jnp.bfloat16)
    return high, (value - high.astype(jnp.float32)).astype(jnp.bfloat16)


def thirds(value):
    high, rest = halves(value)
    low = value - high.astype(jnp.float32) - rest.astype(jnp.float32)
    return high, rest, low.astype(jnp.bfloat16)


def one(left, right, dims):
    return dot(left, right, dims, lax.Precision.DEFAULT)


def dot3(left, right, dims):
    (lh, ll), (rh, rl) = left, right
    (ld,), (rd,) = dims
    return one(jnp.concatenate([lh, lh, ll], axis=ld), jnp.concatenate([rh, rl, rh], axis=rd), dims)


def share_out(core, value, lanes, kept_ref, sent_ref):
    chips, rows, _ = kept_ref.shape
    for q in range(chips):
        for ref, side in ((kept_ref, core), (sent_ref, 1 - core)):
            at = pl.multiple_of((2 * q + side) * rows, rows)
            ref[q, :, lanes] = value[pl.ds(at, rows), :]


def gram_kernel(place_ref, panel_ref, kept_ref, sent_ref, total, cross):
    width = panel_ref.shape[1]
    rows = panel_ref.shape[0] // STEPS
    dims = ((1,), (0,))
    total[...] = jnp.zeros_like(total)
    cross[...] = jnp.zeros_like(cross)

    @pl.loop(0, STEPS)
    def _(c):
        block = panel_ref[pl.ds(pl.multiple_of(c * rows, rows), rows), :]
        high, rest, low = thirds(block)
        high_t, rest_t = halves(block.T)
        total[...] += one(
            jnp.concatenate([high_t, rest_t], axis=1), jnp.concatenate([high, rest], axis=0), dims
        )
        cross[...] += one(
            jnp.concatenate([high_t, high_t], axis=1), jnp.concatenate([rest, low], axis=0), dims
        )

    total[...] = total[...] + (cross[...] + cross[...].T)
    core = place_ref[1]
    first = (place_ref[0] + core == 0).astype(jnp.float32)
    cross[...] = panel_ref[:width] * first
    share_out(core, total, slice(0, width), kept_ref, sent_ref)
    share_out(core, cross, slice(width, 2 * width), kept_ref, sent_ref)


def product_kernel(
    place_ref, trailing_ref, panel_ref, kept_ref, sent_ref,
    trailing, panel, total, edge, semaphores,
):
    width = panel.shape[1]
    rows = panel.shape[0] // STEPS
    core = place_ref[1]
    first = (place_ref[0] + core == 0).astype(jnp.float32)

    def copies(c):
        at = pl.ds(pl.multiple_of(c * rows, rows), rows)
        return (
            pltpu.make_async_copy(trailing_ref.at[at], trailing.at[at], semaphores.at[0, c]),
            pltpu.make_async_copy(panel_ref.at[at], panel.at[at], semaphores.at[1, c]),
        )

    for c in range(STEPS):
        for copy in copies(c):
            copy.start()
    total[...] = jnp.zeros_like(total)

    @pl.loop(0, STEPS)
    def _(c):
        for copy in copies(c):
            copy.wait()
        at = pl.ds(pl.multiple_of(c * rows, rows), rows)
        total[...] += dot3(halves(trailing[at, :].T), halves(panel[at, :]), ((1,), (0,)))

    edge[...] = trailing[:width].T * first
    share_out(core, total, slice(0, width), kept_ref, sent_ref)
    share_out(core, edge, slice(width, 2 * width), kept_ref, sent_ref)


def stream_call(kernel, place, arrays, out, scratch, flops, copies=()):
    vmem = pl.BlockSpec(memory_space=pltpu.VMEM)
    inputs = pl.BlockSpec(memory_space=pl.ANY) if copies else vmem
    return pl.pallas_call(
        kernel,
        out_shape=[jax.ShapeDtypeStruct(out, jnp.float32)] * 2,
        in_specs=[pl.BlockSpec(memory_space=pltpu.SMEM)] + [inputs] * len(arrays),
        out_specs=[vmem] * 2,
        scratch_shapes=[pltpu.VMEM(s, jnp.float32) for s in scratch] + list(copies),
        compiler_params=pltpu.CompilerParams(vmem_limit_bytes=(60 if copies else 24) * 2**20),
        cost_estimate=estimate(flops),
    )(place, *arrays)


def factor_kernel(place_ref, sums_ref, other_ref, band_ref, inv_ref, sign_ref, top_ref, work, whole):
    width = band_ref.shape[0]
    ring, thin, _ = sums_ref.shape
    x, core = place_ref[0], place_ref[1]
    for s in range(ring):
        base = lax.rem(x + ring - s, ring) * (2 * thin)
        whole[pl.ds(pl.multiple_of(base + core * thin, thin), thin), :] = sums_ref[s]
        whole[pl.ds(pl.multiple_of(base + (1 - core) * thin, thin), thin), :] = other_ref[s]
    work[:, :width] = whole[:, :width]
    work[:, width:] = unit_eye(width)
    top_ref[...] = whole[:, width:]
    for k in range(width // NB):
        lo, hi = k * NB, (k + 1) * NB
        done = eliminate(work[lo:hi, lo:hi], False)
        diag = jnp.sum(done[:, :NB] * unit_eye(NB), axis=1, keepdims=True)
        low = done[:, NB:] * lax.rsqrt(diag)
        right = width + hi
        rows = nn(low, work[lo:hi, lo:right])
        work[lo:hi, lo:right] = rows
        if hi < width:
            work[hi:, hi:right] = work[hi:, hi:right] - tn(rows[:, NB : width - lo], rows[:, NB:])

    eye_r = lax.broadcasted_iota(jnp.int32, (width, width), 0)
    eye_c = lax.broadcasted_iota(jnp.int32, (width, width), 1)
    upper = jnp.where(eye_r <= eye_c, work[:, :width], 0.0)
    inv = jnp.where(eye_r >= eye_c, work[:, width:], 0.0)
    diag_q = jnp.sum(top_ref[...] * inv, axis=1, keepdims=True)
    signs = jnp.where(diag_q > 0.0, -1.0, jnp.where(diag_q < 0.0, 1.0, 0.0))
    band_ref[...] = signs * upper
    inv_ref[...] = inv
    row = jnp.sum(jnp.where(eye_r == eye_c, signs, 0.0), axis=0, keepdims=True)
    sign_ref[...] = jnp.broadcast_to(row, sign_ref.shape)


def sweep(work, side, first, last):
    width = work.shape[0]
    index = lax.broadcasted_iota(jnp.int32, (width, 1), 0)

    @pl.loop(first, last)
    def _(k):
        lo = pl.multiple_of(k * NB, NB)
        cols = at_block(k, work[:, :width], NB)
        side[...] = cols
        done = eliminate(side[pl.ds(lo, NB), :], True)
        rows = nn(done[:, NB:], work[pl.ds(lo, NB), :])
        cols = jnp.where((index >= lo) & (index < lo + NB), 0.0, cols)
        work[...] = work[...] - dot3(halves(cols), halves(rows), ((1,), (0,)))
        work[pl.ds(lo, NB), :] = rows


def block_first(top_ref, inv_ref, sign_ref, work, side):
    width = top_ref.shape[0]
    work[:, :width] = unit_eye(width) - nt(inv_ref[...], top_ref[...]) * sign_ref[0:1, :]
    work[:, width:] = unit_eye(width)
    sweep(work, side, 0, width // NB // 2)


def block_second(state_ref, out_ref, work, side):
    width = out_ref.shape[0]
    work[...] = state_ref[...]
    sweep(work, side, width // NB // 2, width // NB)
    out_ref[...] = work[:, width:]


def right_kernel(
    place_ref, cols_ref, other_ref, block_ref, coupling_ref, right_ref, whole
):
    width = block_ref.shape[0]
    ring, piece, _ = cols_ref.shape
    x, core = place_ref[0], place_ref[1]
    for s in range(ring):
        base = lax.rem(x + ring - s, ring) * (2 * piece)
        whole[pl.ds(pl.multiple_of(base + core * piece, piece), piece), :] = cols_ref[s]
        whole[pl.ds(pl.multiple_of(base + (1 - core) * piece, piece), piece), :] = other_ref[s]
    block = halves(block_ref[...])
    x_cols, y_cols = halves(whole[:, :width]), halves(whole[:, width:])
    w = dot3(x_cols, block, ((1,), (0,)))
    w = w - dot3(y_cols, halves(coupling_ref[...]), ((1,), (0,)))
    d = dot3(y_cols, block, ((1,), (1,)))
    high, low = halves(jnp.concatenate([w, d], axis=1).T)
    span = high.shape[0]
    right_ref[:span] = high
    right_ref[span : 2 * span] = low
    right_ref[2 * span :] = high


def update_kernel(
    place_ref, trailing_ref, y_ref, own_ref, up_ref, over_ref, down_ref, right_ref,
    out_ref, tile, result, left, semaphores, done,
):
    count, width = own_ref.shape
    sources = (own_ref, up_ref, over_ref, down_ref)

    def rows_of(step):
        to = lax.rem(place_ref[2] + len(sources) - step, len(sources))
        return pl.ds(pl.multiple_of(to * count, count), count)

    def loading(step):
        return pltpu.make_async_copy(
            trailing_ref.at[rows_of(step)], tile.at[step], semaphores.at[step]
        )

    def storing(step):
        return pltpu.make_async_copy(result.at[step], out_ref.at[rows_of(step)], done.at[step])

    for step in range(len(sources)):
        loading(step).start()

    @pl.loop(0, len(sources))
    def _(step):
        for n, source in enumerate(sources):

            @pl.when(step == n)
            def _():
                high, low = halves(source[...])
                left[:, width : 2 * width] = high
                left[:, 3 * width : 4 * width] = high
                left[:, 5 * width :] = low

        high, low = halves(y_ref[rows_of(step), :])
        left[:, :width] = high
        left[:, 2 * width : 3 * width] = high
        left[:, 4 * width : 5 * width] = low
        loading(step).wait()
        result[step] = tile[step] - one(left[...], right_ref[...], ((1,), (0,)))
        storing(step).start()

    for step in range(len(sources)):
        storing(step).wait()


def local_call(kernel, outs, scratch, *args, **more):
    return pl.pallas_call(
        kernel,
        out_shape=[jax.ShapeDtypeStruct(s, jnp.float32) for s in outs],
        scratch_shapes=[pltpu.VMEM(s, t) for s, t in scratch],
        compiler_params=pltpu.CompilerParams(vmem_limit_bytes=30 * 2**20),
        **more,
    )(*args)


def estimate(flops):
    return pl.CostEstimate(flops=flops, bytes_accessed=2**20, transcendentals=0)


def update_call(place, trailing, y_rows, sources, cols, cols_other, block, coupling):
    count, width = sources[0].shape
    y_n = len(sources)
    span = trailing.shape[1]
    tiles = (y_n, count, span)
    smem = pl.BlockSpec(memory_space=pltpu.SMEM)
    vmem = pl.BlockSpec(memory_space=pltpu.VMEM)
    hbm = pl.BlockSpec(memory_space=pltpu.HBM)
    right = pl.pallas_call(
        right_kernel,
        name="right_kernel",
        out_shape=jax.ShapeDtypeStruct((6 * width, span), jnp.bfloat16),
        in_specs=[smem] + [vmem] * 4,
        out_specs=vmem,
        scratch_shapes=[pltpu.VMEM((span, 2 * width), jnp.float32)],
        compiler_params=pltpu.CompilerParams(vmem_limit_bytes=30 * 2**20),
        cost_estimate=estimate(2 * 10**9),
    )(place, cols, cols_other, block, coupling)
    args = (y_rows, *sources, right)
    return pl.pallas_call(
        update_kernel,
        name="update_kernel",
        out_shape=jax.ShapeDtypeStruct(trailing.shape, jnp.float32),
        in_specs=[smem, hbm] + [vmem] * len(args),
        out_specs=hbm,
        scratch_shapes=[
            pltpu.VMEM(tiles, jnp.float32),
            pltpu.VMEM(tiles, jnp.float32),
            pltpu.VMEM((count, 6 * width), jnp.bfloat16),
            pltpu.SemaphoreType.DMA((y_n,)),
            pltpu.SemaphoreType.DMA((y_n,)),
        ],
        compiler_params=pltpu.CompilerParams(vmem_limit_bytes=30 * 2**20),
        cost_estimate=estimate(2 * 10**9),
    )(place, trailing, *args)


def exchange(x, axis):
    return lax.all_to_all(x, axis, 0, 0, tiled=True)


def to_everyone(x, axis):
    return exchange(jnp.broadcast_to(x[None], (lax.axis_size(axis), *x.shape)), axis)


def shift(x, axis, by):
    n = lax.axis_size(axis)
    return lax.ppermute(x, axis, [(i, (i + by) % n) for i in range(n)])


def around(x, axis):
    found = [x]
    for s in range(1, lax.axis_size(axis)):
        found.append(shift(x, axis, s))
    return found


def scatter_sum(parts, axis):
    n = lax.axis_size(axis)
    me = lax.axis_index(axis)
    total = lax.dynamic_index_in_dim(parts, me, 0, keepdims=False)
    for s in range(1, n):
        to = lax.dynamic_index_in_dim(parts, (me + s) % n, 0, keepdims=False)
        total = total + shift(to, axis, s)
    return total


def pair_sum(kept, sent):
    return kept + shift(sent, "core", 1)


def shards(trailing, panel):
    width = panel.shape[1]
    local_rows = panel.shape[0]
    local_cols = trailing.shape[1]
    x_n, core_n, z_n, y_n = (lax.axis_size(a) for a in ALL)
    x, core, z, y = (lax.axis_index(a) for a in ALL)
    row = x * core_n + core
    rows_n = x_n * core_n
    piece = local_cols // rows_n
    thin = width // rows_n
    first = (row == 0).astype(jnp.float32)
    swap = [
        ((r * z_n + c) * y_n + k, (c * z_n + r) * y_n + k)
        for r in range(rows_n)
        for c in range(z_n)
        for k in range(y_n)
    ]
    place = jnp.stack([x, core, y]).astype(jnp.int32)

    kept, sent = stream_call(
        gram_kernel,
        place,
        [panel],
        (x_n, thin, 2 * width),
        [(width, width)] * 2,
        10**9,
    )
    sums = jnp.stack(around(scatter_sum(pair_sum(kept, sent), "x"), "x"))
    other = shift(sums, "core", 1)

    kept, sent = stream_call(
        product_kernel,
        place,
        [trailing, panel],
        (x_n, piece, 2 * width),
        [trailing.shape, panel.shape] + [(local_cols, width)] * 2,
        2 * 10**9,
        [pltpu.SemaphoreType.DMA((2, STEPS))],
    )
    pieces = scatter_sum(pair_sum(kept, sent), "x")
    mine = lax.dynamic_slice_in_dim(panel, y * local_cols, local_cols, 0)
    to_swap = lax.dynamic_slice_in_dim(panel, y * local_cols + z * piece, piece, 0)
    swapped = lax.ppermute(jnp.concatenate([pieces, to_swap], axis=1), ALL, swap)
    panel_piece = swapped[:, 2 * width :]

    smem = pl.BlockSpec(memory_space=pltpu.SMEM)
    vmem = pl.BlockSpec(memory_space=pltpu.VMEM)
    band, inv, sign, top = local_call(
        factor_kernel,
        [(width, width), (width, width), (8, width), (width, width)],
        [((width, 2 * width), jnp.float32)] * 2,
        place, sums, other,
        in_specs=[smem, vmem, vmem],
        cost_estimate=estimate(3 * 10**9),
    )
    (state,) = local_call(
        block_first,
        [(width, 2 * width)],
        [((width, NB), jnp.float32)],
        top, inv, sign,
        cost_estimate=estimate(2 * 10**9),
    )
    (block,) = local_call(
        block_second,
        [(width, width)],
        [((width, 2 * width), jnp.float32), ((width, NB), jnp.float32)],
        state,
        cost_estimate=estimate(2 * 10**9),
    )
    sign = sign[0:1]

    def reflectors(rows_of_panel, is_first, count):
        at = lax.broadcasted_iota(jnp.int32, (count, width), 0)
        to = lax.broadcasted_iota(jnp.int32, (count, width), 1)
        return nt(rows_of_panel, inv, HIGH) - jnp.where(at + is_first == to, sign, 0.0)

    far = 2 * local_rows

    def products(both):
        return nt(both[:, :width], inv, HIGH) - both[:, width : 2 * width] * sign

    x_block = to_everyone(products(swapped), "z").reshape(local_cols, width)
    y_block = reflectors(mine, jnp.where(row == 0, y * local_cols, far), local_cols)
    y_rows = reflectors(panel, jnp.where(row == 0, 0, far), local_rows)
    y_piece = reflectors(
        panel_piece, jnp.where((z == 0) & (y == 0), row * piece, far), piece
    )
    cols = jnp.stack(around(jnp.concatenate([products(pieces), y_piece], axis=1), "x"))
    cols_other = shift(cols, "core", 1)

    x_block, block = lax.optimization_barrier((x_block, block))
    inner = tn(y_block, x_block)
    inner = lax.dynamic_slice_in_dim(inner, z * (width // z_n), width // z_n, 0)
    inner, x_block = lax.optimization_barrier((inner, x_block))
    for axis in ("y", "core", "x"):
        inner = functools.reduce(jnp.add, around(inner, axis))
    inner = to_everyone(inner, "z").reshape(width, width)
    coupling = tn(block, nn(inner, block))
    sources = around(x_block, "y")

    updated = update_call(place, trailing, y_rows, sources, cols, cols_other, block, coupling)
    return (updated, band)


def solution(mesh):
    finer = Mesh(mesh.devices.reshape(mesh.shape["row"] // 2, 2, 8, 4), ALL)
    placed = (P(("x", "core"), ("z", "y")), P(("x", "core"), None))
    return jax.shard_map(
        shards,
        mesh=finer,
        in_specs=placed,
        out_specs=(P(("x", "core"), ("z", "y")), P()),
        check_vma=False,
    )
```

```python
import functools

import jax
import jax.numpy as jnp
from jax import lax
from jax.experimental import pallas as pl
from jax.experimental.pallas import tpu as pltpu
from jax.sharding import Mesh
from jax.sharding import PartitionSpec as P

ALL = ("x", "core", "z", "y")
NB = 64
WINDOW = 8
WINDOW_FULL = 6
STEPS = 4
HIGHEST = lax.Precision.HIGHEST
HIGH = lax.Precision.HIGH


def dot(left, right, dims, precision):
    return lax.dot_general(
        left, right, (dims, ((), ())), precision=precision, preferred_element_type=jnp.float32
    )


def nn(left, right, precision=HIGHEST):
    return dot(left, right, ((1,), (0,)), precision)


def nt(left, right, precision=HIGHEST):
    return dot(left, right, ((1,), (1,)), precision)


def tn(left, right, precision=HIGHEST):
    return dot(left, right, ((0,), (0,)), precision)


def unit_eye(n):
    rows = lax.broadcasted_iota(jnp.int32, (n, n), 0)
    cols = lax.broadcasted_iota(jnp.int32, (n, n), 1)
    return (rows == cols).astype(jnp.float32)


def at_block(k, value, size):
    found = value[:, :size]
    for j in range(1, value.shape[1] // size):
        found = jnp.where(k == j, value[:, j * size : (j + 1) * size], found)
    return found


def eliminate(block, full):
    count = NB // 8
    window = WINDOW_FULL if full else WINDOW
    aug = jnp.concatenate([block, unit_eye(NB)], axis=1)
    wide = aug.shape[1]
    tiles = [aug[8 * i : 8 * i + 8] for i in range(count)]
    sub = lax.broadcasted_iota(jnp.int32, (8, wide), 0)

    def spread(j, now):
        first = 0 if full else now // 8
        return {i: jnp.broadcast_to(tiles[i][:, j : j + 1], (8, wide)) for i in range(first, count)}

    def line(tile, s):
        return jnp.broadcast_to(tile[s : s + 1], (8, wide))

    ahead = {j: spread(j, 0) for j in range(min(window, NB))}
    for j in range(NB):
        t, s = divmod(j, 8)
        mine = ahead.pop(j)
        inverse = 1.0 / line(mine[t], s)
        where = range(0 if full else t, count)
        factor = {i: mine[i] * inverse for i in where}
        factor[t] = jnp.where(sub != s if full else sub > s, factor[t], 0.0)
        scale = jnp.where(sub == s, inverse, 1.0) if full else None

        def step(tile, i, pivot):
            kept = tile * scale if full and i == t else tile
            return kept - factor[i] * pivot

        pivot = line(tiles[t], s)
        for i in where:
            tiles[i] = step(tiles[i], i, pivot)
        for l in sorted(ahead):
            pivot = line(ahead[l][t], s)
            ahead[l] = {i: step(ahead[l][i], i, pivot) for i in ahead[l] if i in where}
        if j + window < NB:
            ahead[j + window] = spread(j + window, j + 1)
    return jnp.concatenate(tiles, axis=0)


def halves(value):
    high = value.astype(jnp.bfloat16)
    return high, (value - high.astype(jnp.float32)).astype(jnp.bfloat16)


def thirds(value):
    high, rest = halves(value)
    low = value - high.astype(jnp.float32) - rest.astype(jnp.float32)
    return high, rest, low.astype(jnp.bfloat16)


def one(left, right, dims):
    return dot(left, right, dims, lax.Precision.DEFAULT)


def dot3(left, right, dims):
    (lh, ll), (rh, rl) = left, right
    (ld,), (rd,) = dims
    return one(jnp.concatenate([lh, lh, ll], axis=ld), jnp.concatenate([rh, rl, rh], axis=rd), dims)


def share_out(core, value, lanes, kept_ref, sent_ref):
    chips, rows, _ = kept_ref.shape
    for q in range(chips):
        for ref, side in ((kept_ref, core), (sent_ref, 1 - core)):
            at = pl.multiple_of((2 * q + side) * rows, rows)
            ref[q, :, lanes] = value[pl.ds(at, rows), :]


def gram_kernel(place_ref, panel_ref, kept_ref, sent_ref, total, cross):
    width = panel_ref.shape[1]
    rows = panel_ref.shape[0] // STEPS
    dims = ((1,), (0,))
    total[...] = jnp.zeros_like(total)
    cross[...] = jnp.zeros_like(cross)

    @pl.loop(0, STEPS)
    def _(c):
        block = panel_ref[pl.ds(pl.multiple_of(c * rows, rows), rows), :]
        high, rest, low = thirds(block)
        high_t, rest_t = halves(block.T)
        total[...] += one(
            jnp.concatenate([high_t, rest_t], axis=1), jnp.concatenate([high, rest], axis=0), dims
        )
        cross[...] += one(
            jnp.concatenate([high_t, high_t], axis=1), jnp.concatenate([rest, low], axis=0), dims
        )

    total[...] = total[...] + (cross[...] + cross[...].T)
    core = place_ref[1]
    first = (place_ref[0] + core == 0).astype(jnp.float32)
    cross[...] = panel_ref[:width] * first
    share_out(core, total, slice(0, width), kept_ref, sent_ref)
    share_out(core, cross, slice(width, 2 * width), kept_ref, sent_ref)


def product_kernel(
    place_ref, trailing_ref, panel_ref, kept_ref, sent_ref,
    trailing, panel, total, edge, semaphores,
):
    width = panel.shape[1]
    rows = panel.shape[0] // STEPS
    core = place_ref[1]
    first = (place_ref[0] + core == 0).astype(jnp.float32)

    def copies(c):
        at = pl.ds(pl.multiple_of(c * rows, rows), rows)
        return (
            pltpu.make_async_copy(trailing_ref.at[at], trailing.at[at], semaphores.at[0, c]),
            pltpu.make_async_copy(panel_ref.at[at], panel.at[at], semaphores.at[1, c]),
        )

    for c in range(STEPS):
        for copy in copies(c):
            copy.start()
    total[...] = jnp.zeros_like(total)

    @pl.loop(0, STEPS)
    def _(c):
        for copy in copies(c):
            copy.wait()
        at = pl.ds(pl.multiple_of(c * rows, rows), rows)
        total[...] += dot3(halves(trailing[at, :].T), halves(panel[at, :]), ((1,), (0,)))

    edge[...] = trailing[:width].T * first
    share_out(core, total, slice(0, width), kept_ref, sent_ref)
    share_out(core, edge, slice(width, 2 * width), kept_ref, sent_ref)


def stream_call(kernel, place, arrays, out, scratch, flops, copies=()):
    vmem = pl.BlockSpec(memory_space=pltpu.VMEM)
    inputs = pl.BlockSpec(memory_space=pl.ANY) if copies else vmem
    return pl.pallas_call(
        kernel,
        out_shape=[jax.ShapeDtypeStruct(out, jnp.float32)] * 2,
        in_specs=[pl.BlockSpec(memory_space=pltpu.SMEM)] + [inputs] * len(arrays),
        out_specs=[vmem] * 2,
        scratch_shapes=[pltpu.VMEM(s, jnp.float32) for s in scratch] + list(copies),
        compiler_params=pltpu.CompilerParams(vmem_limit_bytes=(60 if copies else 24) * 2**20),
        cost_estimate=estimate(flops),
    )(place, *arrays)


def factor_kernel(place_ref, sums_ref, other_ref, band_ref, inv_ref, sign_ref, top_ref, work, whole):
    width = band_ref.shape[0]
    ring, thin, _ = sums_ref.shape
    x, core = place_ref[0], place_ref[1]
    for s in range(ring):
        base = lax.rem(x + ring - s, ring) * (2 * thin)
        whole[pl.ds(pl.multiple_of(base + core * thin, thin), thin), :] = sums_ref[s]
        whole[pl.ds(pl.multiple_of(base + (1 - core) * thin, thin), thin), :] = other_ref[s]
    work[:, :width] = whole[:, :width]
    work[:, width:] = unit_eye(width)
    top_ref[...] = whole[:, width:]
    for k in range(width // NB):
        lo, hi = k * NB, (k + 1) * NB
        done = eliminate(work[lo:hi, lo:hi], False)
        diag = jnp.sum(done[:, :NB] * unit_eye(NB), axis=1, keepdims=True)
        low = done[:, NB:] * lax.rsqrt(diag)
        right = width + hi
        rows = nn(low, work[lo:hi, lo:right])
        work[lo:hi, lo:right] = rows
        if hi < width:
            work[hi:, hi:right] = work[hi:, hi:right] - tn(rows[:, NB : width - lo], rows[:, NB:])

    eye_r = lax.broadcasted_iota(jnp.int32, (width, width), 0)
    eye_c = lax.broadcasted_iota(jnp.int32, (width, width), 1)
    upper = jnp.where(eye_r <= eye_c, work[:, :width], 0.0)
    inv = jnp.where(eye_r >= eye_c, work[:, width:], 0.0)
    diag_q = jnp.sum(top_ref[...] * inv, axis=1, keepdims=True)
    signs = jnp.where(diag_q > 0.0, -1.0, jnp.where(diag_q < 0.0, 1.0, 0.0))
    band_ref[...] = signs * upper
    inv_ref[...] = inv
    row = jnp.sum(jnp.where(eye_r == eye_c, signs, 0.0), axis=0, keepdims=True)
    sign_ref[...] = jnp.broadcast_to(row, sign_ref.shape)


def sweep(work, side, first, last):
    width = work.shape[0]
    index = lax.broadcasted_iota(jnp.int32, (width, 1), 0)

    @pl.loop(first, last)
    def _(k):
        lo = pl.multiple_of(k * NB, NB)
        cols = at_block(k, work[:, :width], NB)
        side[...] = cols
        done = eliminate(side[pl.ds(lo, NB), :], True)
        rows = nn(done[:, NB:], work[pl.ds(lo, NB), :])
        cols = jnp.where((index >= lo) & (index < lo + NB), 0.0, cols)
        work[...] = work[...] - dot3(halves(cols), halves(rows), ((1,), (0,)))
        work[pl.ds(lo, NB), :] = rows


def block_first(top_ref, inv_ref, sign_ref, work, side):
    width = top_ref.shape[0]
    work[:, :width] = unit_eye(width) - nt(inv_ref[...], top_ref[...]) * sign_ref[0:1, :]
    work[:, width:] = unit_eye(width)
    sweep(work, side, 0, width // NB // 2)


def block_second(state_ref, out_ref, work, side):
    width = out_ref.shape[0]
    work[...] = state_ref[...]
    sweep(work, side, width // NB // 2, width // NB)
    out_ref[...] = work[:, width:]


def right_kernel(
    place_ref, cols_ref, other_ref, block_ref, coupling_ref, right_ref, whole
):
    width = block_ref.shape[0]
    ring, piece, _ = cols_ref.shape
    x, core = place_ref[0], place_ref[1]
    for s in range(ring):
        base = lax.rem(x + ring - s, ring) * (2 * piece)
        whole[pl.ds(pl.multiple_of(base + core * piece, piece), piece), :] = cols_ref[s]
        whole[pl.ds(pl.multiple_of(base + (1 - core) * piece, piece), piece), :] = other_ref[s]
    block = halves(block_ref[...])
    x_cols, y_cols = halves(whole[:, :width]), halves(whole[:, width:])
    w = dot3(x_cols, block, ((1,), (0,)))
    w = w - dot3(y_cols, halves(coupling_ref[...]), ((1,), (0,)))
    d = dot3(y_cols, block, ((1,), (1,)))
    high, low = halves(jnp.concatenate([w, d], axis=1).T)
    span = high.shape[0]
    right_ref[:span] = high
    right_ref[span : 2 * span] = low
    right_ref[2 * span :] = high


def update_kernel(
    place_ref, trailing_ref, y_ref, own_ref, up_ref, over_ref, down_ref, right_ref,
    out_ref, result, left, done,
):
    count, width = own_ref.shape
    sources = (own_ref, up_ref, over_ref, down_ref)

    def rows_of(step):
        to = lax.rem(place_ref[2] + len(sources) - step, len(sources))
        return pl.ds(pl.multiple_of(to * count, count), count)

    def storing(step):
        return pltpu.make_async_copy(result.at[step], out_ref.at[rows_of(step)], done.at[step])

    @pl.loop(0, len(sources))
    def _(step):
        for n, source in enumerate(sources):

            @pl.when(step == n)
            def _():
                high, low = halves(source[...])
                left[:, width : 2 * width] = high
                left[:, 3 * width : 4 * width] = high
                left[:, 5 * width :] = low

        high, low = halves(y_ref[rows_of(step), :])
        left[:, :width] = high
        left[:, 2 * width : 3 * width] = high
        left[:, 4 * width : 5 * width] = low
        tile = trailing_ref[rows_of(step), :]
        result[step] = tile - one(left[...], right_ref[...], ((1,), (0,)))
        storing(step).start()

    for step in range(len(sources)):
        storing(step).wait()


def local_call(kernel, outs, scratch, *args, **more):
    return pl.pallas_call(
        kernel,
        out_shape=[jax.ShapeDtypeStruct(s, jnp.float32) for s in outs],
        scratch_shapes=[pltpu.VMEM(s, t) for s, t in scratch],
        compiler_params=pltpu.CompilerParams(vmem_limit_bytes=30 * 2**20),
        **more,
    )(*args)


def estimate(flops):
    return pl.CostEstimate(flops=flops, bytes_accessed=2**20, transcendentals=0)


def update_call(place, trailing, y_rows, sources, cols, cols_other, block, coupling):
    count, width = sources[0].shape
    y_n = len(sources)
    span = trailing.shape[1]
    tiles = (y_n, count, span)
    smem = pl.BlockSpec(memory_space=pltpu.SMEM)
    vmem = pl.BlockSpec(memory_space=pltpu.VMEM)
    hbm = pl.BlockSpec(memory_space=pltpu.HBM)
    right = pl.pallas_call(
        right_kernel,
        name="right_kernel",
        out_shape=jax.ShapeDtypeStruct((6 * width, span), jnp.bfloat16),
        in_specs=[smem] + [vmem] * 4,
        out_specs=vmem,
        scratch_shapes=[pltpu.VMEM((span, 2 * width), jnp.float32)],
        compiler_params=pltpu.CompilerParams(vmem_limit_bytes=30 * 2**20),
        cost_estimate=estimate(2 * 10**9),
    )(place, cols, cols_other, block, coupling)
    args = (y_rows, *sources, right)
    return pl.pallas_call(
        update_kernel,
        name="update_kernel",
        out_shape=jax.ShapeDtypeStruct(trailing.shape, jnp.float32),
        in_specs=[smem, vmem] + [vmem] * len(args),
        out_specs=hbm,
        scratch_shapes=[
            pltpu.VMEM(tiles, jnp.float32),
            pltpu.VMEM((count, 6 * width), jnp.bfloat16),
            pltpu.SemaphoreType.DMA((y_n,)),
        ],
        compiler_params=pltpu.CompilerParams(vmem_limit_bytes=30 * 2**20),
        cost_estimate=estimate(2 * 10**9),
    )(place, trailing, *args)


def exchange(x, axis):
    return lax.all_to_all(x, axis, 0, 0, tiled=True)


def to_everyone(x, axis):
    return exchange(jnp.broadcast_to(x[None], (lax.axis_size(axis), *x.shape)), axis)


def shift(x, axis, by):
    n = lax.axis_size(axis)
    return lax.ppermute(x, axis, [(i, (i + by) % n) for i in range(n)])


def around(x, axis):
    found = [x]
    for s in range(1, lax.axis_size(axis)):
        found.append(shift(x, axis, s))
    return found


def scatter_sum(parts, axis):
    n = lax.axis_size(axis)
    me = lax.axis_index(axis)
    total = lax.dynamic_index_in_dim(parts, me, 0, keepdims=False)
    for s in range(1, n):
        to = lax.dynamic_index_in_dim(parts, (me + s) % n, 0, keepdims=False)
        total = total + shift(to, axis, s)
    return total


def pair_sum(kept, sent):
    return kept + shift(sent, "core", 1)


def shards(trailing, panel):
    width = panel.shape[1]
    local_rows = panel.shape[0]
    local_cols = trailing.shape[1]
    x_n, core_n, z_n, y_n = (lax.axis_size(a) for a in ALL)
    x, core, z, y = (lax.axis_index(a) for a in ALL)
    row = x * core_n + core
    rows_n = x_n * core_n
    piece = local_cols // rows_n
    thin = width // rows_n
    first = (row == 0).astype(jnp.float32)
    swap = [
        ((r * z_n + c) * y_n + k, (c * z_n + r) * y_n + k)
        for r in range(rows_n)
        for c in range(z_n)
        for k in range(y_n)
    ]
    place = jnp.stack([x, core, y]).astype(jnp.int32)

    kept, sent = stream_call(
        gram_kernel,
        place,
        [panel],
        (x_n, thin, 2 * width),
        [(width, width)] * 2,
        10**9,
    )
    sums = jnp.stack(around(scatter_sum(pair_sum(kept, sent), "x"), "x"))
    other = shift(sums, "core", 1)

    kept, sent = stream_call(
        product_kernel,
        place,
        [trailing, panel],
        (x_n, piece, 2 * width),
        [trailing.shape, panel.shape] + [(local_cols, width)] * 2,
        2 * 10**9,
        [pltpu.SemaphoreType.DMA((2, STEPS))],
    )
    pieces = scatter_sum(pair_sum(kept, sent), "x")
    mine = lax.dynamic_slice_in_dim(panel, y * local_cols, local_cols, 0)
    to_swap = lax.dynamic_slice_in_dim(panel, y * local_cols + z * piece, piece, 0)
    swapped = lax.ppermute(jnp.concatenate([pieces, to_swap], axis=1), ALL, swap)
    panel_piece = swapped[:, 2 * width :]

    smem = pl.BlockSpec(memory_space=pltpu.SMEM)
    vmem = pl.BlockSpec(memory_space=pltpu.VMEM)
    band, inv, sign, top = local_call(
        factor_kernel,
        [(width, width), (width, width), (8, width), (width, width)],
        [((width, 2 * width), jnp.float32)] * 2,
        place, sums, other,
        in_specs=[smem, vmem, vmem],
        cost_estimate=estimate(3 * 10**9),
    )
    (state,) = local_call(
        block_first,
        [(width, 2 * width)],
        [((width, NB), jnp.float32)],
        top, inv, sign,
        cost_estimate=estimate(2 * 10**9),
    )
    (block,) = local_call(
        block_second,
        [(width, width)],
        [((width, 2 * width), jnp.float32), ((width, NB), jnp.float32)],
        state,
        cost_estimate=estimate(2 * 10**9),
    )
    sign = sign[0:1]

    def reflectors(rows_of_panel, is_first, count):
        at = lax.broadcasted_iota(jnp.int32, (count, width), 0)
        to = lax.broadcasted_iota(jnp.int32, (count, width), 1)
        return nt(rows_of_panel, inv, HIGH) - jnp.where(at + is_first == to, sign, 0.0)

    far = 2 * local_rows

    def products(both):
        return nt(both[:, :width], inv, HIGH) - both[:, width : 2 * width] * sign

    x_block = to_everyone(products(swapped), "z").reshape(local_cols, width)
    y_block = reflectors(mine, jnp.where(row == 0, y * local_cols, far), local_cols)
    y_rows = reflectors(panel, jnp.where(row == 0, 0, far), local_rows)
    y_piece = reflectors(
        panel_piece, jnp.where((z == 0) & (y == 0), row * piece, far), piece
    )
    cols = jnp.stack(around(jnp.concatenate([products(pieces), y_piece], axis=1), "x"))
    cols_other = shift(cols, "core", 1)

    x_block, block = lax.optimization_barrier((x_block, block))
    inner = tn(y_block, x_block)
    inner = lax.dynamic_slice_in_dim(inner, z * (width // z_n), width // z_n, 0)
    inner, x_block = lax.optimization_barrier((inner, x_block))
    for axis in ("y", "core", "x"):
        inner = functools.reduce(jnp.add, around(inner, axis))
    inner = to_everyone(inner, "z").reshape(width, width)
    coupling = tn(block, nn(inner, block))
    sources = around(x_block, "y")

    updated = update_call(place, trailing, y_rows, sources, cols, cols_other, block, coupling)
    return (updated, band)


def solution(mesh):
    finer = Mesh(mesh.devices.reshape(mesh.shape["row"] // 2, 2, 8, 4), ALL)
    placed = (P(("x", "core"), ("z", "y")), P(("x", "core"), None))
    return jax.shard_map(
        shards,
        mesh=finer,
        in_specs=placed,
        out_specs=(P(("x", "core"), ("z", "y")), P()),
        check_vma=False,
    )
```
